32 devices in a mesh: grp: 4 (over z), row: 4 (over y, core), col: 2 (over x).
Axes of the slice: x: 2, y: 2, z: 4, core: 2. Of those that a mesh axis runs over, the one named last changes fastest.
Arguments:
- tokens: bfloat16 [2048, 4608], P(('grp', 'row', 'col')), parts along dimension 0, may hold values from -6 to 6
- ln_gain: float32 [4608], replicated, may hold values from 0.1 to 1.9
- w_in: bfloat16 [4608, 12288], P('row', 'col'), may hold values from -0.09375 to 0.09375
- b_in: float32 [12288], P('col'), may hold values from -3 to 3
- w_out: bfloat16 [12288, 4608], P('col', 'row'), may hold values from -0.0546875 to 0.0546875
- b_out: float32 [4608], P('row'), may hold values from -3 to 3
Outputs:
- result: bfloat16 [2048, 4608], P(('grp', 'row', 'col')), parts along dimension 0
The draws below stay inside these ranges and needn't reach their ends.
There are 4 independent parts, one for each index of `grp`. The reference program is written for one: setup_inputs(seed, part) draws one part's arguments, and reference() takes and returns one part's arrays. A program takes and returns all parts, laid end to end along the dimension named above; an argument that names none is the same for every part. Nothing has to cross between parts.
All inputs are finite; a program needn't handle non-finite values.
Results may differ from the reference program's by a relative error of at most 0.0095.
Values may be sent and summed in bfloat16 or wider, within the bound.
A program may use at most 128 MiB of HBM per device.

```python
import jax
import jax.numpy as jnp
from jax import lax

D = 4608
FF = 12288
TOKENS = 512


def block_scale(own_key, dims, pieces, low, top_value):
    def one(position, blocks):
        heights = jax.random.uniform(jax.random.fold_in(jax.random.fold_in(own_key, 6), position), (blocks,), jnp.float32, low / len(pieces), top_value / len(pieces))
        return jnp.repeat(jnp.exp(heights), dims[position] // blocks).reshape((-1,) + (1,) * (len(dims) - position - 1))

    loudness = one(*pieces[0])
    for cut in pieces[1:]:
        loudness = loudness * one(*cut)
    return loudness


def normal_values(rng, shape, width, limit, shards=(), held_as=jnp.bfloat16):
    drawn = width * jax.random.normal(rng, shape, jnp.float32)
    if shards:
        drawn = drawn * block_scale(rng, shape, shards, -0.22, 0.18)
    return jnp.clip(drawn, -limit, limit).astype(held_as)


def setup_inputs(seed: int = 0, part: int = 0) -> dict:
    key_list = jax.random.split(jax.random.key(seed), 7)
    own_keys = jax.random.split(jax.random.fold_in(key_list[6], part), 7)
    tokens = normal_values(own_keys[0], (TOKENS, D), 1.0, 6.0, ((0, 8),))
    ln_gain = jnp.clip(1.0 + 0.18 * jax.random.normal(key_list[1], (D,), jnp.float32), 0.1, 1.9)
    w_in = normal_values(key_list[2], (D, FF), D ** -0.5, 0.09375, ((0, 4), (1, 2)))
    b_in = normal_values(key_list[3], (FF,), 0.5, 3.0, ((0, 2),), jnp.float32)
    w_out = normal_values(key_list[4], (FF, D), FF ** -0.5, 0.0546875, ((0, 2), (1, 4)))
    b_out = normal_values(key_list[5], (D,), 0.5, 3.0, ((0, 4),), jnp.float32)
    return {"tokens": tokens, "ln_gain": ln_gain, "w_in": w_in, "b_in": b_in, "w_out": w_out, "b_out": b_out}


def reference(tokens, ln_gain, w_in, b_in, w_out, b_out):
    values = tokens.astype(jnp.float32)
    row_mean = lax.optimization_barrier(jnp.mean(values, axis=1, keepdims=True))
    centered = values - row_mean
    row_var = lax.optimization_barrier(jnp.mean(centered * centered, axis=1, keepdims=True))
    normed = (centered * jax.lax.rsqrt(row_var + 1e-06) * ln_gain).astype(jnp.bfloat16)
    preact = jnp.dot(normed, w_in, preferred_element_type=jnp.float32) + b_in
    hidden = jax.nn.gelu(preact, approximate=False).astype(jnp.bfloat16)
    branch_out = (jnp.dot(hidden, w_out, preferred_element_type=jnp.float32) + b_out).astype(jnp.bfloat16)
    return (values + branch_out.astype(jnp.float32)).astype(jnp.bfloat16)
```

```python
import jax
import jax.numpy as jnp
from jax import lax
from jax.experimental import pallas as pl
from jax.experimental.pallas import tpu as pltpu
from jax.sharding import PartitionSpec as P

MESH = pl.DeviceIdType.MESH
F32, BF16 = jnp.float32, jnp.bfloat16


QUARTERS = (0, 1, 2, 3, 4)
CHUNKS = (((0, 0),), ((1, 0), (0, 1)), ((1, 1), (1, 2)), ((0, 2), (1, 3)), ((0, 3),))
SLICES = ((1, 1, 2, 2), (3, 3), (3, 3), (3, 3), (2, 2, 2))


def plan(rows):
    spans = [(rows * a // 4, rows * b // 4) for a, b in zip(QUARTERS, QUARTERS[1:])]
    base, starts, at = {}, [], 0
    for chunk in CHUNKS:
        starts.append(at)
        for cc, s in chunk:
            base[cc, s] = at
            at += 4 * (spans[s][1] - spans[s][0])
    return spans, base, starts, [b - a for a, b in zip(starts, starts[1:] + [at])]


def tile_of(size, limit):
    return next(t for t in range(limit, 0, -128) if size % t == 0)


def block_kernel(
    tokens_hbm, gain_hbm, w_in_hbm, b_in_hbm, w_out_hbm, b_out_hbm, out_ref,
    tokens, gain_ref, b_in_ref, b_out_ref, gain, b_in, b_out, w_in, w_out, normed, panel, psend, precv, ssend, srecv, hidden, total,
    okeep, osend, orecv, branch, regrouped,
    v_sem, t_sem, w_sem, send_sem, in_recv, fwd_recv, p_recv, s_recv, h_recv, o_recv, b_recv,
):
    r, c = lax.axis_index("row"), lax.axis_index("col")
    y, k = r // 2, r % 2
    partner, across, diagonal = 2 * y + (1 - k), 2 * (1 - y) + k, 2 * (1 - y) + (1 - k)
    others = (across, diagonal, partner)
    rows, width = tokens.shape
    depth = w_in.shape[0]
    tiles, _, tile = psend.shape
    half = tiles * tile
    spans, base, starts, counts = plan(rows)
    scope = jax.named_scope

    def tall(s):
        return spans[s][1] - spans[s][0]

    def span(s):
        return pl.ds(spans[s][0], tall(s))

    def quads(s):
        return pl.ds(4 * spans[s][0], 4 * tall(s))

    def order(j, i):
        return sum(len(cuts) for cuts in SLICES[:j]) + i

    def part(first, s, q):
        return pl.ds(pl.multiple_of(first + q * tall(s), 8), tall(s))

    def flat(j):
        return pl.ds(starts[j], counts[j])

    def bounds(j, i):
        return tiles * sum(SLICES[j][:i]) // 6, tiles * sum(SLICES[j][: i + 1]) // 6

    def cut(j, i):
        lo, hi = bounds(j, i)
        return pl.ds(lo, hi - lo)

    def remote(src, dst, send, recv, row, col=None):
        target = {"row": row} if col is None else {"row": row, "col": col}
        return pltpu.make_async_remote_copy(
            src_ref=src, dst_ref=dst, send_sem=send, recv_sem=recv, device_id=target, device_id_type=MESH
        )

    def load(which):
        return pltpu.make_async_copy((w_in_hbm, w_out_hbm)[which], (w_in, w_out)[which], w_sem.at[which])

    def fetch(s):
        return pltpu.make_async_copy(tokens_hbm.at[span(s)], tokens.at[span(s)], t_sem.at[s])

    barrier = pltpu.get_barrier_semaphore()
    for target in ({"row": across}, {"row": diagonal}, {"row": partner}, {"col": 1 - c}):
        pl.semaphore_signal(barrier, inc=1, device_id=target, device_id_type=MESH)
    def vector(i):
        src, dst = ((gain_hbm, gain_ref), (b_in_hbm, b_in_ref), (b_out_hbm, b_out_ref))[i]
        return pltpu.make_async_copy(src, dst, v_sem.at[i])

    fetch(0).start()
    vector(0).start()
    for s in range(1, len(spans)):
        fetch(s).start()
    load(0).start()
    vector(1).start()
    vector(2).start()

    def flatten(src, dst, begin, size):
        for i in range(size // 128):
            dst[:, i * 128 : (i + 1) * 128] = src[pl.ds(begin + i, 1), :]

    def normalize(s):
        values = tokens[span(s), :].astype(F32)
        centered = values - jnp.mean(values, axis=1, keepdims=True)
        var = jnp.mean(centered * centered, axis=1, keepdims=True)
        scaled = (centered * lax.rsqrt(var + 1e-06) * gain[...]).astype(BF16)
        for q in range(4):
            normed[q, span(s), :] = scaled[:, q * depth : (q + 1) * depth]

    def piece(s, i):
        return remote(
            normed.at[others[i], span(s)], panel.at[part(base[0, s], s, r)], send_sem.at[0], in_recv.at[s], others[i]
        )

    def forward(s):
        return remote(
            panel.at[pl.ds(base[0, s], 4 * tall(s))], panel.at[pl.ds(base[1, s], 4 * tall(s))],
            send_sem.at[1], fwd_recv.at[s], r, 1 - c,
        )

    def gathered(s):
        held = panel.at[pl.ds(base[0, s], 3 * tall(s))]
        remote(held, held, send_sem.at[0], in_recv.at[s], across).wait_recv()
        forward(s).start()

    def share(j, i):
        return remote(
            psend.at[cut(j, i), flat(j)], precv.at[cut(j, i), flat(j)], send_sem.at[2], p_recv.at[order(j, i)], partner
        )

    def cross(j, i):
        return remote(
            ssend.at[cut(j, i), flat(j)], srecv.at[cut(j, i), flat(j)], send_sem.at[3], s_recv.at[order(j, i)], across
        )

    def spread(j, i, which):
        held = hidden.at[which, cut(j, i), flat(j)]
        return remote(held, held, send_sem.at[4], h_recv.at[order(j, i)], partner)

    def lend(s):
        return remote(osend.at[quads(s)], orecv.at[quads(s)], send_sem.at[5], o_recv.at[s], r, 1 - c)

    def give(s, i):
        q = others[i]
        return remote(
            branch.at[part(4 * spans[s][0], s, q)], regrouped.at[r, span(s)], send_sem.at[6], b_recv.at[s], q
        )

    def each_tile(j, i, body):
        lo, hi = bounds(j, i)
        if hi - lo == 1:
            body(lo)
        else:
            pl.loop(lo, hi)(body)

    def first(j, between=()):
        def columns(core, t):
            return pl.ds(pl.multiple_of(core * half + t * tile, tile), tile)

        def theirs(i):
            def one(t):
                x = panel[flat(j), :]
                psend[t, flat(j), :] = jnp.dot(
                    x, w_in[:, columns(1 - k, t)], preferred_element_type=F32
                ).astype(BF16)

            with scope(f"theirs{j}"):
                each_tile(j, i, one)
            share(j, i).start()

        def ours(i):
            with scope(f"sharewait{j}"):
                share(j, i).wait_recv()

            def one(t):
                x = panel[flat(j), :]
                mine = jnp.dot(x, w_in[:, columns(k, t)], preferred_element_type=F32)
                ssend[t, flat(j), :] = (mine + precv[t, flat(j), :].astype(F32)).astype(BF16)

            with scope(f"ours{j}"):
                each_tile(j, i, one)
            cross(j, i).start()

        count = len(SLICES[j])
        theirs(0)
        for s in between:
            gathered(s)
        for i in range(count):
            if i + 1 < count:
                theirs(i + 1)
            ours(i)

    def second(j):
        acc = total.at[pl.ds(0, counts[j])]
        acc[...] = jnp.zeros((counts[j], depth), F32)
        count = len(SLICES[j])

        def down(i, which):
            def one(t):
                deep = pl.ds(pl.multiple_of(which * half + t * tile, tile), tile)
                acc[...] += jnp.dot(hidden[which, t, flat(j), :], w_out[deep, :], preferred_element_type=F32)

            with scope(f"down{j}"):
                each_tile(j, i, one)

        def theirs(i):
            with scope(f"spreadwait{j}"):
                spread(j, i, 1 - k).wait_recv()
            down(i, 1 - k)

        for i in range(count):
            with scope(f"crosswait{j}"):
                cross(j, i).wait_recv()

            def activate(t):
                bias = b_in[:, pl.ds(pl.multiple_of(t * tile, tile), tile)]
                v = ssend[t, flat(j), :].astype(F32) + srecv[t, flat(j), :].astype(F32) + bias
                hidden[k, t, flat(j), :] = (v * (1.0 + lax.erf(v * (0.5**0.5))) * 0.5).astype(BF16)

            with scope(f"gelu{j}"):
                each_tile(j, i, activate)
            spread(j, i, k).start()
            if j == 0 and i == 0:
                load(1).wait()
            down(i, k)
            if i > 0:
                theirs(i - 1)
        theirs(count - 1)
        for cc, s in sorted(CHUNKS[j], reverse=True):
            held = total[pl.ds(base[cc, s] - starts[j], 4 * tall(s)), :]
            if cc == 0:
                okeep[quads(s), :] = held
            else:
                osend[quads(s), :] = held.astype(BF16)
                lend(s).start()

    def finish(s):
        with scope(f"lendwait{s}"):
            lend(s).wait_recv()
        summed = okeep[quads(s), :] + orecv[quads(s), :].astype(F32) + b_out[...]
        branch[quads(s), :] = summed.astype(BF16)
        for i in range(3):
            give(s, i).start()
        regrouped[r, span(s), :] = branch[part(4 * spans[s][0], s, r), :]

    def settle(s):
        with scope(f"givewait{s}"):
            held = branch.at[pl.ds(0, 3 * tall(s))]
            remote(held, held, send_sem.at[6], b_recv.at[s], across).wait_recv()
        for q in range(4):
            out_ref[span(s), q * depth : (q + 1) * depth] = regrouped[q, span(s), :]

    vector(0).wait()
    flatten(gain_ref, gain, 0, width)
    for s in range(len(spans)):
        with scope(f"fetch{s}"):
            fetch(s).wait()
        with scope(f"norm{s}"):
            normalize(s)
        if s == 0:
            with scope("barrier"):
                pl.semaphore_wait(barrier, 4)
        for i in range(3):
            piece(s, i).start()
        panel[part(base[0, s], s, r), :] = normed[r, span(s), :]

    with scope("inwait0"):
        gathered(0)
    with scope("loadw"):
        load(0).wait()
    load(1).start()
    first(0)
    with scope("inwait1"):
        gathered(1)
    with scope("fwdwait0"):
        forward(0).wait_recv()
    first(1, between=(2, 3))
    with scope("fwdwait1"):
        forward(1).wait_recv()
    with scope("fwdwait2"):
        forward(2).wait_recv()
    first(2)
    with scope("fwdwait3"):
        forward(3).wait_recv()
    first(3)
    first(4)

    vector(1).wait()
    flatten(b_in_ref, b_in, k * (half // 128), half)
    vector(2).wait()
    flatten(b_out_ref, b_out, 0, depth)
    second(0)
    second(1)
    finish(0)
    second(2)
    finish(1)
    second(3)
    finish(2)
    second(4)
    finish(3)
    for s in range(len(spans)):
        settle(s)

    with scope("drain"):
        sent = (
            normed.at[pl.ds(0, 3)], panel.at[pl.ds(0, 4 * rows)], psend, ssend, hidden.at[k], osend,
            branch.at[pl.ds(0, 3 * rows)],
        )
        for i, held in enumerate(sent):
            remote(held, held, send_sem.at[i], send_sem.at[i], across).wait_send()


def fused(tokens, ln_gain, w_in, b_in, w_out, b_out):
    rows, width = tokens.shape
    depth, units = w_in.shape
    half = units // 2
    tile = tile_of(half, 512)
    spans, _, _, counts = plan(rows)
    many, cuts = len(spans), sum(len(cuts) for cuts in SLICES)
    vmem, dma = pltpu.VMEM, pltpu.SemaphoreType.DMA
    in_vmem, in_hbm = pl.BlockSpec(memory_space=vmem), pl.BlockSpec(memory_space=pl.ANY)
    stage = vmem((half // tile, 8 * rows, tile), BF16)
    branch_out = pl.pallas_call(
        block_kernel,
        out_shape=pltpu.VMEM((rows, width), BF16),
        in_specs=[in_hbm] * 6,
        out_specs=in_vmem,
        scratch_shapes=[
            vmem((rows, width), BF16),
            vmem((width // 128, 128), F32),
            vmem((units // 128, 128), F32),
            vmem((depth // 128, 128), F32),
            vmem((1, width), F32),
            vmem((1, half), F32),
            vmem((1, depth), F32),
            vmem(w_in.shape, BF16),
            vmem(w_out.shape, BF16),
            vmem((4, rows, depth), BF16),
            vmem((8 * rows, depth), BF16),
            stage,
            stage,
            stage,
            stage,
            vmem((2, half // tile, 8 * rows, tile), BF16),
            vmem((max(counts), depth), F32),
            vmem((4 * rows, depth), F32),
            vmem((4 * rows, depth), BF16),
            vmem((4 * rows, depth), BF16),
            vmem((4 * rows, depth), BF16),
            vmem((4, rows, depth), BF16),
            dma((3,)),
            dma((many,)),
            dma((2,)),
            dma((7,)),
            dma((many,)),
            dma((many,)),
            dma((cuts,)),
            dma((cuts,)),
            dma((cuts,)),
            dma((many,)),
            dma((many,)),
        ],
        compiler_params=pltpu.CompilerParams(
            collective_id=0, has_side_effects=True, vmem_limit_bytes=62000000
        ),
        name="mlp_block",
    )(tokens, ln_gain.reshape(-1, 128), w_in, b_in.reshape(-1, 128), w_out, b_out.reshape(-1, 128))
    return (tokens.astype(F32) + branch_out.astype(F32)).astype(BF16)


def local(tokens, ln_gain, w_in, b_in, w_out, b_out):
    values = tokens.astype(jnp.float32)
    row_mean = jnp.mean(values, axis=1, keepdims=True)
    centered = values - row_mean
    row_var = jnp.mean(centered * centered, axis=1, keepdims=True)
    normed = (centered * lax.rsqrt(row_var + 1e-06) * ln_gain).astype(jnp.bfloat16)
    own_cols = lax.all_to_all(normed, "row", split_axis=1, concat_axis=0, tiled=True)
    partial_pre = jnp.dot(
        lax.all_gather(own_cols, "col", axis=0, tiled=True),
        w_in,
        preferred_element_type=jnp.float32,
    )
    preact = lax.psum_scatter(partial_pre, "row", scatter_dimension=0, tiled=True) + b_in
    hidden = jax.nn.gelu(preact, approximate=False).astype(jnp.bfloat16)
    down_part = jnp.dot(
        lax.all_gather(hidden, "row", axis=0, tiled=True), w_out, preferred_element_type=jnp.float32
    )
    summed = lax.psum_scatter(
        down_part.astype(jnp.bfloat16), "col", scatter_dimension=0, tiled=True
    ).astype(jnp.float32)
    branch_out = (summed + b_out).astype(jnp.bfloat16)
    regrouped = lax.all_to_all(branch_out, "row", split_axis=0, concat_axis=1, tiled=True)
    return (values + regrouped.astype(jnp.float32)).astype(jnp.bfloat16)


def solution(mesh):
    in_specs = (
        P(("grp", "row", "col"), None),
        P(),
        P("row", "col"),
        P("col"),
        P("col", "row"),
        P("row"),
    )
    out_specs = P(("grp", "row", "col"), None)
    body = fused if (mesh.shape["row"], mesh.shape["col"]) == (4, 2) else local
    return jax.shard_map(body, mesh=mesh, in_specs=in_specs, out_specs=out_specs, check_vma=False)
```

```python
import jax
import jax.numpy as jnp
from jax import lax
from jax.experimental import pallas as pl
from jax.experimental.pallas import tpu as pltpu
from jax.sharding import PartitionSpec as P

MESH = pl.DeviceIdType.MESH
F32, BF16 = jnp.float32, jnp.bfloat16


QUARTERS = (0, 1, 2, 3, 4)
CHUNKS = (((0, 0),), ((1, 0), (0, 1)), ((1, 1), (1, 2)), ((0, 2), (1, 3)), ((0, 3),))
SLICES = ((1, 1, 2, 2), (3, 3), (3, 3), (3, 3), (2, 2, 2))
TAKEN = ((6,), (6,), (6,), (3, 3), (2, 2, 2))


def plan(rows):
    spans = [(rows * a // 4, rows * b // 4) for a, b in zip(QUARTERS, QUARTERS[1:])]
    base, starts, at = {}, [], 0
    for chunk in CHUNKS:
        starts.append(at)
        for cc, s in chunk:
            base[cc, s] = at
            at += 4 * (spans[s][1] - spans[s][0])
    return spans, base, starts, [b - a for a, b in zip(starts, starts[1:] + [at])]


def tile_of(size, limit):
    return next(t for t in range(limit, 0, -128) if size % t == 0)


def block_kernel(
    tokens_hbm, gain_hbm, w_in_hbm, b_in_hbm, w_out_hbm, b_out_hbm, out_ref,
    tokens, gain_ref, b_in_ref, b_out_ref, gain, b_in, b_out, w_in, w_out, normed, panel, psend, precv, ssend, srecv, hidden, total,
    okeep, osend, orecv, branch, regrouped,
    v_sem, t_sem, w_sem, send_sem, in_recv, fwd_recv, p_recv, s_recv, h_recv, o_recv, b_recv,
):
    r, c = lax.axis_index("row"), lax.axis_index("col")
    y, k = r // 2, r % 2
    partner, across, diagonal = 2 * y + (1 - k), 2 * (1 - y) + k, 2 * (1 - y) + (1 - k)
    others = (across, diagonal, partner)
    rows, width = tokens.shape
    depth = w_in.shape[0]
    tiles, _, tile = psend.shape
    half = tiles * tile
    spans, base, starts, counts = plan(rows)
    scope = jax.named_scope

    def tall(s):
        return spans[s][1] - spans[s][0]

    def span(s):
        return pl.ds(spans[s][0], tall(s))

    def quads(s):
        return pl.ds(4 * spans[s][0], 4 * tall(s))

    def part(first, s, q):
        return pl.ds(pl.multiple_of(first + q * tall(s), 8), tall(s))

    def flat(j):
        return pl.ds(starts[j], counts[j])

    def bounds(slices, j, i):
        return tiles * sum(slices[j][:i]) // 6, tiles * sum(slices[j][: i + 1]) // 6

    def cut(slices, j, i):
        lo, hi = bounds(slices, j, i)
        return pl.ds(lo, hi - lo)

    def order(slices, j, i):
        return sum(len(cuts) for cuts in slices[:j]) + i

    def taken(j, i):
        lo = bounds(SLICES, j, i)[0]
        return next(n for n in range(len(TAKEN[j])) if lo < bounds(TAKEN, j, n)[1])

    def remote(src, dst, send, recv, row, col=None):
        target = {"row": row} if col is None else {"row": row, "col": col}
        return pltpu.make_async_remote_copy(
            src_ref=src, dst_ref=dst, send_sem=send, recv_sem=recv, device_id=target, device_id_type=MESH
        )

    def load(which):
        return pltpu.make_async_copy((w_in_hbm, w_out_hbm)[which], (w_in, w_out)[which], w_sem.at[which])

    def fetch(i):
        at = (span(0), pl.ds(spans[0][1], rows - spans[0][1]))[i]
        return pltpu.make_async_copy(tokens_hbm.at[at], tokens.at[at], t_sem.at[i])

    barrier = pltpu.get_barrier_semaphore()
    for target in ({"row": across}, {"row": diagonal}, {"row": partner}, {"col": 1 - c}):
        pl.semaphore_signal(barrier, inc=1, device_id=target, device_id_type=MESH)
    def vector(i):
        src, dst = ((gain_hbm, gain_ref), (b_in_hbm, b_in_ref), (b_out_hbm, b_out_ref))[i]
        return pltpu.make_async_copy(src, dst, v_sem.at[i])

    fetch(0).start()
    vector(0).start()
    fetch(1).start()
    load(0).start()
    vector(1).start()
    vector(2).start()

    def flatten(src, dst, begin, size):
        for i in range(size // 128):
            dst[:, i * 128 : (i + 1) * 128] = src[pl.ds(begin + i, 1), :]

    def normalize(s):
        values = tokens[span(s), :].astype(F32)
        centered = values - jnp.mean(values, axis=1, keepdims=True)
        var = jnp.mean(centered * centered, axis=1, keepdims=True)
        scaled = (centered * lax.rsqrt(var + 1e-06) * gain[...]).astype(BF16)
        for q in range(4):
            normed[q, span(s), :] = scaled[:, q * depth : (q + 1) * depth]

    def piece(s, i):
        return remote(
            normed.at[others[i], span(s)], panel.at[part(base[0, s], s, r)], send_sem.at[0], in_recv.at[s], others[i]
        )

    def forward(s):
        return remote(
            panel.at[pl.ds(base[0, s], 4 * tall(s))], panel.at[pl.ds(base[1, s], 4 * tall(s))],
            send_sem.at[1], fwd_recv.at[s], r, 1 - c,
        )

    def gathered(s):
        held = panel.at[pl.ds(base[0, s], 3 * tall(s))]
        remote(held, held, send_sem.at[0], in_recv.at[s], across).wait_recv()
        forward(s).start()

    def share(j, i):
        at = (cut(SLICES, j, i), flat(j))
        return remote(psend.at[at], precv.at[at], send_sem.at[2], p_recv.at[order(SLICES, j, i) % 4], partner)

    def cross(j, at, n):
        at = (at, flat(j))
        return remote(ssend.at[at], srecv.at[at], send_sem.at[3], s_recv.at[order(TAKEN, j, n)], across)

    def spread(j, i, which):
        held = hidden.at[which, cut(TAKEN, j, i), flat(j)]
        return remote(held, held, send_sem.at[4], h_recv.at[order(TAKEN, j, i)], partner)

    def lend(s):
        return remote(osend.at[quads(s)], orecv.at[quads(s)], send_sem.at[5], o_recv.at[s], r, 1 - c)

    def give(s, i):
        q = others[i]
        return remote(
            branch.at[part(4 * spans[s][0], s, q)], regrouped.at[r, span(s)], send_sem.at[6], b_recv.at[s], q
        )

    def each_tile(slices, j, i, body):
        lo, hi = bounds(slices, j, i)
        if hi - lo == 1:
            body(lo)
        else:
            pl.loop(lo, hi)(body)

    def first(j, between=()):
        def columns(core, t):
            return pl.ds(pl.multiple_of(core * half + t * tile, tile), tile)

        def theirs(i):
            def one(t):
                x = panel[flat(j), :]
                psend[t, flat(j), :] = jnp.dot(
                    x, w_in[:, columns(1 - k, t)], preferred_element_type=F32
                ).astype(BF16)

            with scope(f"theirs{j}"):
                each_tile(SLICES, j, i, one)
            share(j, i).start()

        def ours(i):
            with scope(f"sharewait{j}"):
                share(j, i).wait_recv()

            def one(t):
                x = panel[flat(j), :]
                mine = jnp.dot(x, w_in[:, columns(k, t)], preferred_element_type=F32)
                ssend[t, flat(j), :] = (mine + precv[t, flat(j), :].astype(F32)).astype(BF16)

            with scope(f"ours{j}"):
                each_tile(SLICES, j, i, one)
            cross(j, cut(SLICES, j, i), taken(j, i)).start()

        count = len(SLICES[j])
        theirs(0)
        for s in between:
            gathered(s)
        for i in range(count):
            if i + 1 < count:
                theirs(i + 1)
            ours(i)

    def second(j):
        acc = total.at[pl.ds(0, counts[j])]
        acc[...] = jnp.zeros((counts[j], depth), F32)
        count = len(TAKEN[j])

        def down(i, which):
            def one(t):
                deep = pl.ds(pl.multiple_of(which * half + t * tile, tile), tile)
                acc[...] += jnp.dot(hidden[which, t, flat(j), :], w_out[deep, :], preferred_element_type=F32)

            with scope(f"down{j}"):
                each_tile(TAKEN, j, i, one)

        def theirs(i):
            with scope(f"spreadwait{j}"):
                spread(j, i, 1 - k).wait_recv()
            down(i, 1 - k)

        for i in range(count):
            with scope(f"crosswait{j}"):
                cross(j, cut(TAKEN, j, i), i).wait_recv()

            def activate(t):
                bias = b_in[:, pl.ds(pl.multiple_of(t * tile, tile), tile)]
                v = ssend[t, flat(j), :].astype(F32) + srecv[t, flat(j), :].astype(F32) + bias
                hidden[k, t, flat(j), :] = (v * (1.0 + lax.erf(v * (0.5**0.5))) * 0.5).astype(BF16)

            with scope(f"gelu{j}"):
                each_tile(TAKEN, j, i, activate)
            spread(j, i, k).start()
            if j == 0 and i == 0:
                load(1).wait()
            down(i, k)
            if i > 0:
                theirs(i - 1)
        theirs(count - 1)
        for cc, s in sorted(CHUNKS[j], reverse=True):
            held = total[pl.ds(base[cc, s] - starts[j], 4 * tall(s)), :]
            if cc == 0:
                okeep[quads(s), :] = held
            else:
                osend[quads(s), :] = held.astype(BF16)
                lend(s).start()

    def finish(s):
        with scope(f"lendwait{s}"):
            lend(s).wait_recv()
        summed = okeep[quads(s), :] + orecv[quads(s), :].astype(F32) + b_out[...]
        branch[quads(s), :] = summed.astype(BF16)
        for i in range(3):
            give(s, i).start()
        regrouped[r, span(s), :] = branch[part(4 * spans[s][0], s, r), :]

    def settle(s):
        with scope(f"givewait{s}"):
            held = branch.at[pl.ds(0, 3 * tall(s))]
            remote(held, held, send_sem.at[6], b_recv.at[s], across).wait_recv()
        for q in range(4):
            at = pl.ds(q * depth, depth)
            out_ref[span(s), at] = (
                tokens[span(s), at].astype(F32) + regrouped[q, span(s), :].astype(F32)
            ).astype(BF16)

    vector(0).wait()
    flatten(gain_ref, gain, 0, width)
    for s in range(len(spans)):
        if s < 2:
            with scope(f"fetch{s}"):
                fetch(s).wait()
        with scope(f"norm{s}"):
            normalize(s)
        if s == 0:
            with scope("barrier"):
                pl.semaphore_wait(barrier, 4)
        for i in range(3):
            piece(s, i).start()
        panel[part(base[0, s], s, r), :] = normed[r, span(s), :]

    with scope("inwait0"):
        gathered(0)
    with scope("loadw"):
        load(0).wait()
    load(1).start()
    first(0)
    with scope("inwait1"):
        gathered(1)
    with scope("fwdwait0"):
        forward(0).wait_recv()
    first(1, between=(2, 3))
    with scope("fwdwait1"):
        forward(1).wait_recv()
    with scope("fwdwait2"):
        forward(2).wait_recv()
    first(2)
    with scope("fwdwait3"):
        forward(3).wait_recv()
    first(3)
    first(4)

    vector(1).wait()
    flatten(b_in_ref, b_in, k * (half // 128), half)
    vector(2).wait()
    flatten(b_out_ref, b_out, 0, depth)
    second(0)
    second(1)
    finish(0)
    second(2)
    finish(1)
    second(3)
    finish(2)
    second(4)
    finish(3)
    for s in range(len(spans)):
        settle(s)

    with scope("drain"):
        sent = (
            normed.at[pl.ds(0, 3)], panel.at[pl.ds(0, 4 * rows)], psend, ssend, hidden.at[k], osend,
            branch.at[pl.ds(0, 3 * rows)],
        )
        for i, held in enumerate(sent):
            remote(held, held, send_sem.at[i], send_sem.at[i], across).wait_send()


def fused(tokens, ln_gain, w_in, b_in, w_out, b_out):
    rows, width = tokens.shape
    depth, units = w_in.shape
    half = units // 2
    tile = tile_of(half, 512)
    spans, _, _, counts = plan(rows)
    many, cuts = len(spans), sum(len(slices) for slices in TAKEN)
    vmem, dma = pltpu.VMEM, pltpu.SemaphoreType.DMA
    in_vmem, in_hbm = pl.BlockSpec(memory_space=vmem), pl.BlockSpec(memory_space=pl.ANY)
    stage = vmem((half // tile, 8 * rows, tile), BF16)
    return pl.pallas_call(
        block_kernel,
        out_shape=pltpu.VMEM((rows, width), BF16),
        in_specs=[in_hbm] * 6,
        out_specs=in_vmem,
        scratch_shapes=[
            vmem((rows, width), BF16),
            vmem((width // 128, 128), F32),
            vmem((units // 128, 128), F32),
            vmem((depth // 128, 128), F32),
            vmem((1, width), F32),
            vmem((1, half), F32),
            vmem((1, depth), F32),
            vmem(w_in.shape, BF16),
            vmem(w_out.shape, BF16),
            vmem((4, rows, depth), BF16),
            vmem((8 * rows, depth), BF16),
            stage,
            stage,
            stage,
            stage,
            vmem((2, half // tile, 8 * rows, tile), BF16),
            vmem((max(counts), depth), F32),
            vmem((4 * rows, depth), F32),
            vmem((4 * rows, depth), BF16),
            vmem((4 * rows, depth), BF16),
            vmem((4 * rows, depth), BF16),
            vmem((4, rows, depth), BF16),
            dma((3,)),
            dma((2,)),
            dma((2,)),
            dma((7,)),
            dma((many,)),
            dma((many,)),
            dma((4,)),
            dma((cuts,)),
            dma((cuts,)),
            dma((many,)),
            dma((many,)),
        ],
        compiler_params=pltpu.CompilerParams(
            collective_id=0, has_side_effects=True, vmem_limit_bytes=62000000
        ),
        name="mlp_block",
    )(tokens, ln_gain.reshape(-1, 128), w_in, b_in.reshape(-1, 128), w_out, b_out.reshape(-1, 128))


def local(tokens, ln_gain, w_in, b_in, w_out, b_out):
    values = tokens.astype(jnp.float32)
    row_mean = jnp.mean(values, axis=1, keepdims=True)
    centered = values - row_mean
    row_var = jnp.mean(centered * centered, axis=1, keepdims=True)
    normed = (centered * lax.rsqrt(row_var + 1e-06) * ln_gain).astype(jnp.bfloat16)
    own_cols = lax.all_to_all(normed, "row", split_axis=1, concat_axis=0, tiled=True)
    partial_pre = jnp.dot(
        lax.all_gather(own_cols, "col", axis=0, tiled=True),
        w_in,
        preferred_element_type=jnp.float32,
    )
    preact = lax.psum_scatter(partial_pre, "row", scatter_dimension=0, tiled=True) + b_in
    hidden = jax.nn.gelu(preact, approximate=False).astype(jnp.bfloat16)
    down_part = jnp.dot(
        lax.all_gather(hidden, "row", axis=0, tiled=True), w_out, preferred_element_type=jnp.float32
    )
    summed = lax.psum_scatter(
        down_part.astype(jnp.bfloat16), "col", scatter_dimension=0, tiled=True
    ).astype(jnp.float32)
    branch_out = (summed + b_out).astype(jnp.bfloat16)
    regrouped = lax.all_to_all(branch_out, "row", split_axis=0, concat_axis=1, tiled=True)
    return (values + regrouped.astype(jnp.float32)).astype(jnp.bfloat16)


def solution(mesh):
    in_specs = (
        P(("grp", "row", "col"), None),
        P(),
        P("row", "col"),
        P("col"),
        P("col", "row"),
        P("row"),
    )
    out_specs = P(("grp", "row", "col"), None)
    body = fused if (mesh.shape["row"], mesh.shape["col"]) == (4, 2) else local
    return jax.shard_map(body, mesh=mesh, in_specs=in_specs, out_specs=out_specs, check_vma=False)
```

```python
import jax
import jax.numpy as jnp
from jax import lax
from jax.experimental import pallas as pl
from jax.experimental.pallas import tpu as pltpu
from jax.sharding import PartitionSpec as P

MESH = pl.DeviceIdType.MESH
F32, BF16 = jnp.float32, jnp.bfloat16


QUARTERS = (0, 1, 2, 3, 4)
CHUNKS = (((0, 0),), ((1, 0), (0, 1)), ((1, 1), (1, 2)), ((0, 2), (1, 3)), ((0, 3),))
SLICES = ((1, 1, 2, 2), (3, 3), (3, 3), (3, 3), (2, 2, 2))
PAIRED = (0, 1, 1, 2)
TAKEN = ((6,), (6,), (6,), (3, 3), (2, 2, 2))


def plan(rows):
    spans = [(rows * a // 4, rows * b // 4) for a, b in zip(QUARTERS, QUARTERS[1:])]
    base, starts, at = {}, [], 0
    for chunk in CHUNKS:
        starts.append(at)
        for cc, s in chunk:
            base[cc, s] = at
            at += 4 * (spans[s][1] - spans[s][0])
    return spans, base, starts, [b - a for a, b in zip(starts, starts[1:] + [at])]


def tile_of(size, limit):
    return next(t for t in range(limit, 0, -128) if size % t == 0)


def block_kernel(
    tokens_hbm, gain_hbm, w_in_hbm, b_in_hbm, w_out_hbm, b_out_hbm, out_ref,
    tokens, gain_ref, b_in_ref, b_out_ref, gain, b_in, b_out, w_in, w_out, normed, panel, psend, precv, ssend, srecv, hidden, total,
    okeep, osend, orecv, branch, regrouped,
    v_sem, t_sem, w_sem, send_sem, in_recv, fwd_recv, p_recv, s_recv, h_recv, o_recv,
):
    r, c = lax.axis_index("row"), lax.axis_index("col")
    y, k = r // 2, r % 2
    partner, across, diagonal = 2 * y + (1 - k), 2 * (1 - y) + k, 2 * (1 - y) + (1 - k)
    others = (2 * (1 - y), 2 * (1 - y) + 1, partner)
    rows, width = tokens.shape
    depth = w_in.shape[0]
    tiles, _, tile = psend.shape
    half = tiles * tile
    spans, base, starts, counts = plan(rows)
    last = len(spans) - 1
    scope = jax.named_scope

    def tall(s):
        return spans[s][1] - spans[s][0]

    def span(s):
        return pl.ds(spans[s][0], tall(s))

    def quads(s):
        return pl.ds(4 * spans[s][0], 4 * tall(s))

    def part(first, s, q):
        return pl.ds(pl.multiple_of(first + q * tall(s), 8), tall(s))

    def flat(j):
        return pl.ds(starts[j], counts[j])

    def bounds(slices, j, i):
        return tiles * sum(slices[j][:i]) // 6, tiles * sum(slices[j][: i + 1]) // 6

    def cut(slices, j, i):
        lo, hi = bounds(slices, j, i)
        return pl.ds(lo, hi - lo)

    def order(slices, j, i):
        return sum(len(cuts) for cuts in slices[:j]) + i

    def taken(j, i):
        lo = bounds(SLICES, j, i)[0]
        return next(n for n in range(len(TAKEN[j])) if lo < bounds(TAKEN, j, n)[1])

    def remote(src, dst, send, recv, row, col=None):
        target = {"row": row} if col is None else {"row": row, "col": col}
        return pltpu.make_async_remote_copy(
            src_ref=src, dst_ref=dst, send_sem=send, recv_sem=recv, device_id=target, device_id_type=MESH
        )

    def load(which):
        return pltpu.make_async_copy((w_in_hbm, w_out_hbm)[which], (w_in, w_out)[which], w_sem)

    def fetch(i):
        at = (span(0), pl.ds(spans[0][1], rows - spans[0][1]))[i]
        return pltpu.make_async_copy(tokens_hbm.at[at], tokens.at[at], t_sem.at[i])

    barrier = pltpu.get_barrier_semaphore()
    for target in ({"row": across}, {"row": diagonal}, {"row": partner}, {"col": 1 - c}):
        pl.semaphore_signal(barrier, inc=1, device_id=target, device_id_type=MESH)
    def vector(i):
        src, dst = ((gain_hbm, gain_ref), (b_in_hbm, b_in_ref), (b_out_hbm, b_out_ref))[i]
        return pltpu.make_async_copy(src, dst, v_sem)

    fetch(0).start()
    vector(0).start()
    fetch(1).start()
    load(0).start()

    def flatten(src, dst, begin, size):
        for i in range(size // 128):
            dst[:, i * 128 : (i + 1) * 128] = src[pl.ds(begin + i, 1), :]

    def normalize(s):
        values = tokens[span(s), :].astype(F32)
        centered = values - jnp.mean(values, axis=1, keepdims=True)
        var = jnp.mean(centered * centered, axis=1, keepdims=True)
        scaled = (centered * lax.rsqrt(var + 1e-06) * gain[...]).astype(BF16)
        for q in range(4):
            normed[q, span(s), :] = scaled[:, q * depth : (q + 1) * depth]

    def piece(s, i):
        return remote(
            normed.at[others[i], span(s)], panel.at[part(base[0, s], s, r)], send_sem.at[0], in_recv.at[min(s, 1)], others[i]
        )

    def forward(s):
        return remote(
            panel.at[pl.ds(base[0, s], 4 * tall(s))], panel.at[pl.ds(base[1, s], 4 * tall(s))],
            send_sem.at[1], fwd_recv.at[PAIRED[s]], r, 1 - c,
        )

    def gathered(which, count):
        held = panel.at[pl.ds(0, 3 * count)]
        remote(held, held, send_sem.at[0], in_recv.at[which], across).wait_recv()

    def passed(sem, which, *among):
        held = panel.at[pl.ds(0, 4 * sum(tall(s) for s in among))]
        remote(held, held, send_sem.at[1], sem.at[which], r, 1 - c).wait_recv()

    def share(j, i):
        at = (cut(SLICES, j, i), flat(j))
        return remote(psend.at[at], precv.at[at], send_sem.at[2], p_recv.at[order(SLICES, j, i) % 4], partner)

    def cross(j, at, n):
        at = (at, flat(j))
        return remote(ssend.at[at], srecv.at[at], send_sem.at[2], s_recv.at[order(TAKEN, j, n)], across)

    def spread(j, i, which):
        held = hidden.at[which, cut(TAKEN, j, i), flat(j)]
        return remote(held, held, send_sem.at[3], h_recv.at[order(TAKEN, j, i) % 4], partner)

    def lend(s):
        return remote(osend.at[quads(s)], orecv.at[quads(s)], send_sem.at[1], o_recv.at[PAIRED[s]], r, 1 - c)

    def give(s, i):
        q = others[i]
        return remote(
            branch.at[part(4 * spans[s][0], s, q)], regrouped.at[r, span(s)], send_sem.at[0], in_recv.at[s // last], q
        )

    def each_tile(slices, j, i, body):
        lo, hi = bounds(slices, j, i)
        if hi - lo == 1:
            body(lo)
        else:
            pl.loop(lo, hi)(body)

    def first(j):
        def columns(core, t):
            return pl.ds(pl.multiple_of(core * half + t * tile, tile), tile)

        def theirs(i):
            def one(t):
                x = panel[flat(j), :]
                psend[t, flat(j), :] = jnp.dot(
                    x, w_in[:, columns(1 - k, t)], preferred_element_type=F32
                ).astype(BF16)

            with scope(f"theirs{j}"):
                each_tile(SLICES, j, i, one)
            share(j, i).start()

        def ours(i):
            with scope(f"sharewait{j}"):
                share(j, i).wait_recv()

            def one(t):
                x = panel[flat(j), :]
                mine = jnp.dot(x, w_in[:, columns(k, t)], preferred_element_type=F32)
                ssend[t, flat(j), :] = (mine + precv[t, flat(j), :].astype(F32)).astype(BF16)

            with scope(f"ours{j}"):
                each_tile(SLICES, j, i, one)
            cross(j, cut(SLICES, j, i), taken(j, i)).start()

        count = len(SLICES[j])
        theirs(0)
        for i in range(count):
            if i + 1 < count:
                theirs(i + 1)
            ours(i)

    def second(j):
        acc = total.at[pl.ds(0, counts[j])]
        acc[...] = jnp.zeros((counts[j], depth), F32)
        count = len(TAKEN[j])

        def down(i, which):
            def one(t):
                deep = pl.ds(pl.multiple_of(which * half + t * tile, tile), tile)
                acc[...] += jnp.dot(hidden[which, t, flat(j), :], w_out[deep, :], preferred_element_type=F32)

            with scope(f"down{j}"):
                each_tile(TAKEN, j, i, one)

        def theirs(i):
            with scope(f"spreadwait{j}"):
                spread(j, i, 1 - k).wait_recv()
            down(i, 1 - k)

        for i in range(count):
            with scope(f"crosswait{j}"):
                cross(j, cut(TAKEN, j, i), i).wait_recv()

            def activate(t):
                bias = b_in[:, pl.ds(pl.multiple_of(t * tile, tile), tile)]
                v = ssend[t, flat(j), :].astype(F32) + srecv[t, flat(j), :].astype(F32) + bias
                hidden[k, t, flat(j), :] = (v * (1.0 + lax.erf(v * (0.5**0.5))) * 0.5).astype(BF16)

            with scope(f"gelu{j}"):
                each_tile(TAKEN, j, i, activate)
            spread(j, i, k).start()
            if j == 0 and i == 0:
                load(1).wait()
            down(i, k)
            if i > 0:
                theirs(i - 1)
        theirs(count - 1)
        for cc, s in sorted(CHUNKS[j], reverse=True):
            held = total[pl.ds(base[cc, s] - starts[j], 4 * tall(s)), :]
            if cc == 0:
                okeep[quads(s), :] = held
            else:
                osend[quads(s), :] = held.astype(BF16)
                lend(s).start()

    def finish(s):
        summed = okeep[quads(s), :] + orecv[quads(s), :].astype(F32) + b_out[...]
        branch[quads(s), :] = summed.astype(BF16)
        for i in range(3):
            give(s, i).start()
        regrouped[r, span(s), :] = branch[part(4 * spans[s][0], s, r), :]

    def settle(s):
        for q in range(4):
            at = pl.ds(q * depth, depth)
            out_ref[span(s), at] = (
                tokens[span(s), at].astype(F32) + regrouped[q, span(s), :].astype(F32)
            ).astype(BF16)

    vector(0).wait()
    vector(1).start()
    flatten(gain_ref, gain, 0, width)
    for s in range(len(spans)):
        if s < 2:
            with scope(f"fetch{s}"):
                fetch(s).wait()
        with scope(f"norm{s}"):
            normalize(s)
        if s == 0:
            with scope("barrier"):
                pl.semaphore_wait(barrier, 4)
        for i in range(3):
            piece(s, i).start()
        panel[part(base[0, s], s, r), :] = normed[r, span(s), :]

    with scope("inwait0"):
        gathered(0, tall(0))
    forward(0).start()
    with scope("loadw"):
        load(0).wait()
    load(1).start()
    first(0)
    with scope("inwait1"):
        gathered(1, rows - tall(0))
    for s in range(1, last + 1):
        forward(s).start()
    with scope("fwdwait0"):
        passed(fwd_recv, 0, 0)
    first(1)
    with scope("fwdwait1"):
        passed(fwd_recv, 1, 1, 2)
    first(2)
    with scope("fwdwait3"):
        passed(fwd_recv, 2, 3)
    first(3)
    first(4)

    vector(1).wait()
    vector(2).start()
    flatten(b_in_ref, b_in, k * (half // 128), half)
    second(0)
    second(1)
    vector(2).wait()
    flatten(b_out_ref, b_out, 0, depth)
    with scope("lendwait0"):
        passed(o_recv, 0, 0)
    finish(0)
    second(2)
    with scope("lendwait1"):
        passed(o_recv, 1, 1, 2)
    finish(1)
    second(3)
    finish(2)
    second(4)
    with scope("lendwait3"):
        passed(o_recv, 2, 3)
    finish(3)
    with scope("givewait0"):
        gathered(0, rows - tall(last))
    for s in range(last):
        settle(s)
    with scope("givewait3"):
        gathered(1, tall(last))
    settle(last)

    with scope("drain"):
        for i, held in enumerate((panel.at[pl.ds(0, 6 * rows)], panel, hidden, psend)):
            remote(held, held, send_sem.at[i], send_sem.at[i], across).wait_send()


def fused(tokens, ln_gain, w_in, b_in, w_out, b_out):
    rows, width = tokens.shape
    depth, units = w_in.shape
    half = units // 2
    tile = tile_of(half, 512)
    spans, _, _, counts = plan(rows)
    cuts = sum(len(slices) for slices in TAKEN)
    vmem, dma = pltpu.VMEM, pltpu.SemaphoreType.DMA
    in_vmem, in_hbm = pl.BlockSpec(memory_space=vmem), pl.BlockSpec(memory_space=pl.ANY)
    stage = vmem((half // tile, 8 * rows, tile), BF16)
    return pl.pallas_call(
        block_kernel,
        out_shape=pltpu.VMEM((rows, width), BF16),
        in_specs=[in_hbm] * 6,
        out_specs=in_vmem,
        scratch_shapes=[
            vmem((rows, width), BF16),
            vmem((width // 128, 128), F32),
            vmem((units // 128, 128), F32),
            vmem((depth // 128, 128), F32),
            vmem((1, width), F32),
            vmem((1, half), F32),
            vmem((1, depth), F32),
            vmem(w_in.shape, BF16),
            vmem(w_out.shape, BF16),
            vmem((4, rows, depth), BF16),
            vmem((8 * rows, depth), BF16),
            stage,
            stage,
            stage,
            stage,
            vmem((2, half // tile, 8 * rows, tile), BF16),
            vmem((max(counts), depth), F32),
            vmem((4 * rows, depth), F32),
            vmem((4 * rows, depth), BF16),
            vmem((4 * rows, depth), BF16),
            vmem((4 * rows, depth), BF16),
            vmem((4, rows, depth), BF16),
            dma,
            dma((2,)),
            dma,
            dma((4,)),
            dma((2,)),
            dma((3,)),
            dma((4,)),
            dma((cuts,)),
            dma((4,)),
            dma((3,)),
        ],
        compiler_params=pltpu.CompilerParams(
            collective_id=0, has_side_effects=True, vmem_limit_bytes=62000000
        ),
        name="mlp_block",
    )(tokens, ln_gain.reshape(-1, 128), w_in, b_in.reshape(-1, 128), w_out, b_out.reshape(-1, 128))


def local(tokens, ln_gain, w_in, b_in, w_out, b_out):
    values = tokens.astype(jnp.float32)
    row_mean = jnp.mean(values, axis=1, keepdims=True)
    centered = values - row_mean
    row_var = jnp.mean(centered * centered, axis=1, keepdims=True)
    normed = (centered * lax.rsqrt(row_var + 1e-06) * ln_gain).astype(jnp.bfloat16)
    own_cols = lax.all_to_all(normed, "row", split_axis=1, concat_axis=0, tiled=True)
    partial_pre = jnp.dot(
        lax.all_gather(own_cols, "col", axis=0, tiled=True),
        w_in,
        preferred_element_type=jnp.float32,
    )
    preact = lax.psum_scatter(partial_pre, "row", scatter_dimension=0, tiled=True) + b_in
    hidden = jax.nn.gelu(preact, approximate=False).astype(jnp.bfloat16)
    down_part = jnp.dot(
        lax.all_gather(hidden, "row", axis=0, tiled=True), w_out, preferred_element_type=jnp.float32
    )
    summed = lax.psum_scatter(
        down_part.astype(jnp.bfloat16), "col", scatter_dimension=0, tiled=True
    ).astype(jnp.float32)
    branch_out = (summed + b_out).astype(jnp.bfloat16)
    regrouped = lax.all_to_all(branch_out, "row", split_axis=0, concat_axis=1, tiled=True)
    return (values + regrouped.astype(jnp.float32)).astype(jnp.bfloat16)


def solution(mesh):
    in_specs = (
        P(("grp", "row", "col"), None),
        P(),
        P("row", "col"),
        P("col"),
        P("col", "row"),
        P("row"),
    )
    out_specs = P(("grp", "row", "col"), None)
    body = fused if (mesh.shape["row"], mesh.shape["col"]) == (4, 2) else local
    return jax.shard_map(body, mesh=mesh, in_specs=in_specs, out_specs=out_specs, check_vma=False)
```

```python
import jax
import jax.numpy as jnp
from jax import lax
from jax.experimental import pallas as pl
from jax.experimental.pallas import tpu as pltpu
from jax.sharding import PartitionSpec as P

MESH = pl.DeviceIdType.MESH
F32, BF16 = jnp.float32, jnp.bfloat16


QUARTERS = (0, 1, 2, 3, 4)
CHUNKS = (((0, 0),), ((1, 0), (0, 1)), ((1, 1), (1, 2)), ((0, 2), (1, 3)), ((0, 3),))
SLICES = ((1, 1, 2, 2), (3, 3), (3, 3), (3, 3), (2, 2, 2))
TAKEN = ((6,), (6,), (6,), (3, 3), (2, 2, 2))


def plan(rows):
    spans = [(rows * a // 4, rows * b // 4) for a, b in zip(QUARTERS, QUARTERS[1:])]
    base, starts, at = {}, [], 0
    for chunk in CHUNKS:
        starts.append(at)
        for cc, s in chunk:
            base[cc, s] = at
            at += 4 * (spans[s][1] - spans[s][0])
    return spans, base, starts, [b - a for a, b in zip(starts, starts[1:] + [at])]


def tile_of(size, limit):
    return next(t for t in range(limit, 0, -128) if size % t == 0)


def block_kernel(
    tokens_hbm, gain_hbm, w_in_hbm, b_in_hbm, w_out_hbm, b_out_hbm, out_ref,
    tokens, gain_ref, b_in_ref, b_out_ref, gain, b_in, b_out, w_in, w_out, normed, panel, psend, precv, ssend, srecv, hidden, total,
    okeep, osend, orecv, branch, regrouped,
    t_sem, w_sem, send_sem, in_recv, fwd_recv, p_recv, s_recv, h_recv, o_recv,
):
    r, c = lax.axis_index("row"), lax.axis_index("col")
    y, k = r // 2, r % 2
    partner, across, diagonal = 2 * y + (1 - k), 2 * (1 - y) + k, 2 * (1 - y) + (1 - k)
    others = (2 * (1 - y), 2 * (1 - y) + 1, partner)
    rows, width = tokens.shape
    depth = w_in.shape[0]
    tiles, _, tile = psend.shape
    half = tiles * tile
    spans, base, starts, counts = plan(rows)
    last = len(spans) - 1
    scope = jax.named_scope

    def tall(s):
        return spans[s][1] - spans[s][0]

    def span(s):
        return pl.ds(spans[s][0], tall(s))

    def quads(s):
        return pl.ds(4 * spans[s][0], 4 * tall(s))

    def part(first, s, q):
        return pl.ds(pl.multiple_of(first + q * tall(s), 8), tall(s))

    def flat(j):
        return pl.ds(starts[j], counts[j])

    def bounds(slices, j, i):
        return tiles * sum(slices[j][:i]) // 6, tiles * sum(slices[j][: i + 1]) // 6

    def cut(slices, j, i):
        lo, hi = bounds(slices, j, i)
        return pl.ds(lo, hi - lo)

    def order(slices, j, i):
        return sum(len(cuts) for cuts in slices[:j]) + i

    def taken(j, i):
        lo = bounds(SLICES, j, i)[0]
        return next(n for n in range(len(TAKEN[j])) if lo < bounds(TAKEN, j, n)[1])

    def remote(src, dst, send, recv, row, col=None):
        target = {"row": row} if col is None else {"row": row, "col": col}
        return pltpu.make_async_remote_copy(
            src_ref=src, dst_ref=dst, send_sem=send, recv_sem=recv, device_id=target, device_id_type=MESH
        )

    def load(which):
        return pltpu.make_async_copy((w_in_hbm, w_out_hbm)[which], (w_in, w_out)[which], w_sem)

    def fetch(i):
        at = (span(0), pl.ds(spans[0][1], rows - spans[0][1]))[i]
        return pltpu.make_async_copy(tokens_hbm.at[at], tokens.at[at], t_sem.at[i])

    barrier = pltpu.get_barrier_semaphore()
    for target in ({"row": across}, {"row": diagonal}, {"row": partner}, {"col": 1 - c}):
        pl.semaphore_signal(barrier, inc=1, device_id=target, device_id_type=MESH)
    def vector(i):
        src, dst = ((gain_hbm, gain_ref), (b_in_hbm, b_in_ref), (b_out_hbm, b_out_ref))[i]
        return pltpu.make_async_copy(src, dst, w_sem)

    fetch(0).start()
    vector(0).start()
    fetch(1).start()

    def flatten(src, dst, begin, size):
        for i in range(size // 128):
            dst[:, i * 128 : (i + 1) * 128] = src[pl.ds(begin + i, 1), :]

    def mean(x):
        parts = [x[:, at : at + 128] for at in range(0, width, 128)]
        while len(parts) > 1:
            parts = [sum(parts[i + 1 : i + 2], parts[i]) for i in range(0, len(parts), 2)]
        return jnp.sum(parts[0], axis=1, keepdims=True) * (1.0 / width)

    def normalize(s):
        values = tokens[span(s), :].astype(F32)
        centered = values - mean(values)
        var = mean(centered * centered)
        scaled = (centered * lax.rsqrt(var + 1e-06) * gain[...]).astype(BF16)
        for q in range(4):
            normed[q, span(s), :] = scaled[:, q * depth : (q + 1) * depth]

    def piece(s, i):
        return remote(
            normed.at[others[i], span(s)], panel.at[part(base[0, s], s, r)], send_sem.at[0], in_recv.at[min(s, 1)], others[i]
        )

    def forward(s):
        return remote(
            panel.at[pl.ds(base[0, s], 4 * tall(s))], panel.at[pl.ds(base[1, s], 4 * tall(s))],
            send_sem.at[1], fwd_recv.at[min(s, 1)], r, 1 - c,
        )

    def gathered(which, count):
        held = panel.at[pl.ds(0, 3 * count)]
        remote(held, held, send_sem.at[0], in_recv.at[which], across).wait_recv()

    def passed(sem, which, *among):
        held = panel.at[pl.ds(0, 4 * sum(tall(s) for s in among))]
        remote(held, held, send_sem.at[1], sem.at[which], r, 1 - c).wait_recv()

    def share(j, i):
        at = (cut(SLICES, j, i), flat(j))
        return remote(psend.at[at], precv.at[at], send_sem.at[2], p_recv.at[order(SLICES, j, i) % 4], partner)

    def cross(j, at, n):
        at = (at, flat(j))
        return remote(ssend.at[at], srecv.at[at], send_sem.at[2], s_recv.at[order(TAKEN, j, n)], across)

    def spread(j, i, which):
        held = hidden.at[which, cut(TAKEN, j, i), flat(j)]
        return remote(held, held, send_sem.at[3], h_recv.at[order(TAKEN, j, i) % 4], partner)

    def lend(s):
        return remote(osend.at[quads(s)], orecv.at[quads(s)], send_sem.at[1], o_recv.at[s // last], r, 1 - c)

    def give(s, i):
        q = others[i]
        return remote(
            branch.at[part(4 * spans[s][0], s, q)], regrouped.at[r, span(s)], send_sem.at[0], in_recv.at[s // last], q
        )

    def each_tile(slices, j, i, body):
        lo, hi = bounds(slices, j, i)
        if hi - lo == 1:
            body(lo)
        else:
            pl.loop(lo, hi)(body)

    def first(j):
        def columns(core, t):
            return pl.ds(pl.multiple_of(core * half + t * tile, tile), tile)

        def theirs(i):
            def one(t):
                x = panel[flat(j), :]
                psend[t, flat(j), :] = jnp.dot(
                    x, w_in[:, columns(1 - k, t)], preferred_element_type=F32
                ).astype(BF16)

            with scope(f"theirs{j}"):
                each_tile(SLICES, j, i, one)
            share(j, i).start()

        def ours(i):
            with scope(f"sharewait{j}"):
                share(j, i).wait_recv()

            def one(t):
                x = panel[flat(j), :]
                mine = jnp.dot(x, w_in[:, columns(k, t)], preferred_element_type=F32)
                ssend[t, flat(j), :] = (mine + precv[t, flat(j), :].astype(F32)).astype(BF16)

            with scope(f"ours{j}"):
                each_tile(SLICES, j, i, one)
            cross(j, cut(SLICES, j, i), taken(j, i)).start()

        count = len(SLICES[j])
        theirs(0)
        for i in range(count):
            if i + 1 < count:
                theirs(i + 1)
            ours(i)

    def second(j):
        acc = total.at[pl.ds(0, counts[j])]
        acc[...] = jnp.zeros((counts[j], depth), F32)
        count = len(TAKEN[j])

        def down(i, which):
            def one(t):
                deep = pl.ds(pl.multiple_of(which * half + t * tile, tile), tile)
                acc[...] += jnp.dot(hidden[which, t, flat(j), :], w_out[deep, :], preferred_element_type=F32)

            with scope(f"down{j}"):
                each_tile(TAKEN, j, i, one)

        def theirs(i):
            with scope(f"spreadwait{j}"):
                spread(j, i, 1 - k).wait_recv()
            down(i, 1 - k)

        for i in range(count):
            with scope(f"crosswait{j}"):
                cross(j, cut(TAKEN, j, i), i).wait_recv()

            def activate(t):
                bias = b_in[:, pl.ds(pl.multiple_of(t * tile, tile), tile)]
                v = ssend[t, flat(j), :].astype(F32) + srecv[t, flat(j), :].astype(F32) + bias
                hidden[k, t, flat(j), :] = (v * (1.0 + lax.erf(v * (0.5**0.5))) * 0.5).astype(BF16)

            with scope(f"gelu{j}"):
                each_tile(TAKEN, j, i, activate)
            spread(j, i, k).start()
            if j == 0 and i == 0:
                load(1).wait()
                vector(2).start()
            down(i, k)
            if i > 0:
                theirs(i - 1)
        theirs(count - 1)
        for cc, s in sorted(CHUNKS[j], reverse=True):
            held = total[pl.ds(base[cc, s] - starts[j], 4 * tall(s)), :]
            if cc == 0:
                okeep[quads(s), :] = held
            else:
                osend[quads(s), :] = held.astype(BF16)
                lend(s).start()

    def finish(s):
        summed = okeep[quads(s), :] + orecv[quads(s), :].astype(F32) + b_out[...]
        branch[quads(s), :] = summed.astype(BF16)
        for i in range(3):
            give(s, i).start()
        regrouped[r, span(s), :] = branch[part(4 * spans[s][0], s, r), :]

    def settle(s):
        for q in range(4):
            at = pl.ds(q * depth, depth)
            out_ref[span(s), at] = (
                tokens[span(s), at].astype(F32) + regrouped[q, span(s), :].astype(F32)
            ).astype(BF16)

    vector(0).wait()
    load(0).start()
    flatten(gain_ref, gain, 0, width)
    for s in range(len(spans)):
        if s < 2:
            with scope(f"fetch{s}"):
                fetch(s).wait()
        with scope(f"norm{s}"):
            normalize(s)
        if s == 0:
            with scope("barrier"):
                pl.semaphore_wait(barrier, 4)
        for i in range(3):
            piece(s, i).start()
        panel[part(base[0, s], s, r), :] = normed[r, span(s), :]

    with scope("inwait0"):
        gathered(0, tall(0))
    forward(0).start()
    with scope("loadw"):
        load(0).wait()
    vector(1).start()
    first(0)
    vector(1).wait()
    load(1).start()
    with scope("inwait1"):
        gathered(1, rows - tall(0))
    for s in range(1, last + 1):
        forward(s).start()
    with scope("fwdwait0"):
        passed(fwd_recv, 0, 0)
    first(1)
    with scope("fwdwait1"):
        passed(fwd_recv, 1, *range(1, last + 1))
    first(2)
    first(3)
    first(4)

    flatten(b_in_ref, b_in, k * (half // 128), half)
    second(0)
    second(1)
    vector(2).wait()
    flatten(b_out_ref, b_out, 0, depth)
    second(2)
    with scope("lendwait0"):
        passed(o_recv, 0, *range(last))
    finish(0)
    finish(1)
    second(3)
    finish(2)
    second(4)
    with scope("lendwait3"):
        passed(o_recv, 1, last)
    finish(3)
    with scope("givewait0"):
        gathered(0, rows - tall(last))
    for s in range(last):
        settle(s)
    with scope("givewait3"):
        gathered(1, tall(last))
    settle(last)

    with scope("drain"):
        for i, held in enumerate((panel.at[pl.ds(0, 6 * rows)], panel, hidden, psend)):
            remote(held, held, send_sem.at[i], send_sem.at[i], across).wait_send()


def fused(tokens, ln_gain, w_in, b_in, w_out, b_out):
    rows, width = tokens.shape
    depth, units = w_in.shape
    half = units // 2
    tile = tile_of(half, 512)
    spans, _, _, counts = plan(rows)
    cuts = sum(len(slices) for slices in TAKEN)
    vmem, dma = pltpu.VMEM, pltpu.SemaphoreType.DMA
    in_vmem, in_hbm = pl.BlockSpec(memory_space=vmem), pl.BlockSpec(memory_space=pl.ANY)
    stage = vmem((half // tile, 8 * rows, tile), BF16)
    return pl.pallas_call(
        block_kernel,
        out_shape=pltpu.VMEM((rows, width), BF16),
        in_specs=[in_hbm] * 6,
        out_specs=in_vmem,
        scratch_shapes=[
            vmem((rows, width), BF16),
            vmem((width // 128, 128), F32),
            vmem((units // 128, 128), F32),
            vmem((depth // 128, 128), F32),
            vmem((1, width), F32),
            vmem((1, half), F32),
            vmem((1, depth), F32),
            vmem(w_in.shape, BF16),
            vmem(w_out.shape, BF16),
            vmem((4, rows, depth), BF16),
            vmem((8 * rows, depth), BF16),
            stage,
            stage,
            stage,
            stage,
            vmem((2, half // tile, 8 * rows, tile), BF16),
            vmem((max(counts), depth), F32),
            vmem((4 * rows, depth), F32),
            vmem((4 * rows, depth), BF16),
            vmem((4 * rows, depth), BF16),
            vmem((4 * rows, depth), BF16),
            vmem((4, rows, depth), BF16),
            dma((2,)),
            dma,
            dma((4,)),
            dma((2,)),
            dma((2,)),
            dma((4,)),
            dma((cuts,)),
            dma((4,)),
            dma((2,)),
        ],
        compiler_params=pltpu.CompilerParams(
            collective_id=0, has_side_effects=True, vmem_limit_bytes=62000000
        ),
        name="mlp_block",
    )(tokens, ln_gain.reshape(-1, 128), w_in, b_in.reshape(-1, 128), w_out, b_out.reshape(-1, 128))


def local(tokens, ln_gain, w_in, b_in, w_out, b_out):
    values = tokens.astype(jnp.float32)
    row_mean = jnp.mean(values, axis=1, keepdims=True)
    centered = values - row_mean
    row_var = jnp.mean(centered * centered, axis=1, keepdims=True)
    normed = (centered * lax.rsqrt(row_var + 1e-06) * ln_gain).astype(jnp.bfloat16)
    own_cols = lax.all_to_all(normed, "row", split_axis=1, concat_axis=0, tiled=True)
    partial_pre = jnp.dot(
        lax.all_gather(own_cols, "col", axis=0, tiled=True),
        w_in,
        preferred_element_type=jnp.float32,
    )
    preact = lax.psum_scatter(partial_pre, "row", scatter_dimension=0, tiled=True) + b_in
    hidden = jax.nn.gelu(preact, approximate=False).astype(jnp.bfloat16)
    down_part = jnp.dot(
        lax.all_gather(hidden, "row", axis=0, tiled=True), w_out, preferred_element_type=jnp.float32
    )
    summed = lax.psum_scatter(
        down_part.astype(jnp.bfloat16), "col", scatter_dimension=0, tiled=True
    ).astype(jnp.float32)
    branch_out = (summed + b_out).astype(jnp.bfloat16)
    regrouped = lax.all_to_all(branch_out, "row", split_axis=0, concat_axis=1, tiled=True)
    return (values + regrouped.astype(jnp.float32)).astype(jnp.bfloat16)


def solution(mesh):
    in_specs = (
        P(("grp", "row", "col"), None),
        P(),
        P("row", "col"),
        P("col"),
        P("col", "row"),
        P("row"),
    )
    out_specs = P(("grp", "row", "col"), None)
    body = fused if (mesh.shape["row"], mesh.shape["col"]) == (4, 2) else local
    return jax.shard_map(body, mesh=mesh, in_specs=in_specs, out_specs=out_specs, check_vma=False)
```

```python
import jax
import jax.numpy as jnp
from jax import lax
from jax.experimental import pallas as pl
from jax.experimental.pallas import tpu as pltpu
from jax.sharding import PartitionSpec as P

MESH = pl.DeviceIdType.MESH
F32, BF16 = jnp.float32, jnp.bfloat16


QUARTERS = (0, 1, 2, 3, 4)
CHUNKS = (((0, 0),), ((1, 0), (0, 1)), ((1, 1), (1, 2)), ((0, 2), (1, 3)), ((0, 3),))
SLICES = ((1, 1, 2, 2), (3, 3), (3, 3), (3, 3), (2, 2, 2))
PAIRED = (0, 1, 1, 2)
TAKEN = ((6,), (6,), (6,), (3, 3), (2, 2, 2))


def plan(rows):
    spans = [(rows * a // 4, rows * b // 4) for a, b in zip(QUARTERS, QUARTERS[1:])]
    base, starts, at = {}, [], 0
    for chunk in CHUNKS:
        starts.append(at)
        for cc, s in chunk:
            base[cc, s] = at
            at += 4 * (spans[s][1] - spans[s][0])
    return spans, base, starts, [b - a for a, b in zip(starts, starts[1:] + [at])]


def tile_of(size, limit):
    return next(t for t in range(limit, 0, -128) if size % t == 0)


def block_kernel(
    tokens_hbm, gain_hbm, w_in_hbm, b_in_hbm, w_out_hbm, b_out_hbm, out_ref,
    tokens, gain_ref, b_in_ref, b_out_ref, gain, b_in, b_out, w_in, w_out, normed, panel, psend, precv, ssend, srecv, hidden, total,
    okeep, osend, orecv, branch, regrouped,
    v_sem, t_sem, w_sem, send_sem, in_recv, fwd_recv, p_recv, s_recv, h_recv, o_recv,
):
    r, c = lax.axis_index("row"), lax.axis_index("col")
    y, k = r // 2, r % 2
    partner, across, diagonal = 2 * y + (1 - k), 2 * (1 - y) + k, 2 * (1 - y) + (1 - k)
    h = (k + y) % 2
    others = (2 * (1 - y), 2 * (1 - y) + 1, partner)
    rows, width = tokens.shape
    depth = w_in.shape[0]
    tiles, _, tile = psend.shape
    half = tiles * tile
    spans, base, starts, counts = plan(rows)
    last = len(spans) - 1
    scope = jax.named_scope

    def tall(s):
        return spans[s][1] - spans[s][0]

    def span(s):
        return pl.ds(spans[s][0], tall(s))

    def quads(s):
        return pl.ds(4 * spans[s][0], 4 * tall(s))

    def part(first, s, q):
        return pl.ds(pl.multiple_of(first + q * tall(s), 8), tall(s))

    def flat(j):
        return pl.ds(starts[j], counts[j])

    def bounds(slices, j, i):
        return tiles * sum(slices[j][:i]) // 6, tiles * sum(slices[j][: i + 1]) // 6

    def cut(slices, j, i):
        lo, hi = bounds(slices, j, i)
        return pl.ds(lo, hi - lo)

    def order(slices, j, i):
        return sum(len(cuts) for cuts in slices[:j]) + i

    def taken(j, i):
        lo = bounds(SLICES, j, i)[0]
        return next(n for n in range(len(TAKEN[j])) if lo < bounds(TAKEN, j, n)[1])

    def remote(src, dst, send, recv, row, col=None):
        target = {"row": row} if col is None else {"row": row, "col": col}
        return pltpu.make_async_remote_copy(
            src_ref=src, dst_ref=dst, send_sem=send, recv_sem=recv, device_id=target, device_id_type=MESH
        )

    def load(which):
        return pltpu.make_async_copy((w_in_hbm, w_out_hbm)[which], (w_in, w_out)[which], w_sem)

    def fetch(i):
        at = (span(0), pl.ds(spans[0][1], rows - spans[0][1]))[i]
        return pltpu.make_async_copy(tokens_hbm.at[at], tokens.at[at], t_sem.at[i])

    barrier = pltpu.get_barrier_semaphore()
    for target in ({"row": across}, {"row": diagonal}, {"row": partner}, {"col": 1 - c}):
        pl.semaphore_signal(barrier, inc=1, device_id=target, device_id_type=MESH)
    def vector(i):
        src, dst = ((gain_hbm, gain_ref), (b_in_hbm, b_in_ref), (b_out_hbm, b_out_ref))[i]
        return pltpu.make_async_copy(src, dst, v_sem)

    fetch(0).start()
    vector(0).start()
    fetch(1).start()
    load(0).start()

    def flatten(src, dst, begin, size):
        for i in range(size // 128):
            dst[:, i * 128 : (i + 1) * 128] = src[pl.ds(begin + i, 1), :]

    def normalize(s):
        values = tokens[span(s), :].astype(F32)
        centered = values - jnp.mean(values, axis=1, keepdims=True)
        var = jnp.mean(centered * centered, axis=1, keepdims=True)
        scaled = (centered * lax.rsqrt(var + 1e-06) * gain[...]).astype(BF16)
        for q in range(4):
            normed[q, span(s), :] = scaled[:, q * depth : (q + 1) * depth]

    def piece(s, i):
        return remote(
            normed.at[others[i], span(s)], panel.at[part(base[0, s], s, r)], send_sem.at[0], in_recv.at[min(s, 1)], others[i]
        )

    def forward(s):
        return remote(
            panel.at[pl.ds(base[0, s], 4 * tall(s))], panel.at[pl.ds(base[1, s], 4 * tall(s))],
            send_sem.at[1], fwd_recv.at[PAIRED[s]], r, 1 - c,
        )

    def gathered(which, count):
        held = panel.at[pl.ds(0, 3 * count)]
        remote(held, held, send_sem.at[0], in_recv.at[which], across).wait_recv()

    def passed(sem, which, *among):
        held = panel.at[pl.ds(0, 4 * sum(tall(s) for s in among))]
        remote(held, held, send_sem.at[1], sem.at[which], r, 1 - c).wait_recv()

    def share(j, i):
        at = (cut(SLICES, j, i), flat(j))
        return remote(psend.at[at], precv.at[at], send_sem.at[2], p_recv.at[order(SLICES, j, i) % 4], partner)

    def cross(j, at, n):
        at = (at, flat(j))
        return remote(ssend.at[at], srecv.at[at], send_sem.at[2], s_recv.at[order(TAKEN, j, n)], diagonal)

    def spread(j, i, which):
        held = hidden.at[which, cut(TAKEN, j, i), flat(j)]
        return remote(held, held, send_sem.at[3], h_recv.at[order(TAKEN, j, i) % 4], partner)

    def lend(s):
        return remote(osend.at[quads(s)], orecv.at[quads(s)], send_sem.at[1], o_recv.at[PAIRED[s]], r, 1 - c)

    def give(s, i):
        q = others[i]
        return remote(
            branch.at[part(4 * spans[s][0], s, q)], regrouped.at[r, span(s)], send_sem.at[0], in_recv.at[s // last], q
        )

    def each_tile(slices, j, i, body):
        lo, hi = bounds(slices, j, i)
        if hi - lo == 1:
            body(lo)
        else:
            pl.loop(lo, hi)(body)

    def first(j):
        def columns(core, t):
            return pl.ds(pl.multiple_of(core * half + t * tile, tile), tile)

        def theirs(i):
            def one(t):
                x = panel[flat(j), :]
                psend[t, flat(j), :] = jnp.dot(
                    x, w_in[:, columns(1 - h, t)], preferred_element_type=F32
                ).astype(BF16)

            with scope(f"theirs{j}"):
                each_tile(SLICES, j, i, one)
            share(j, i).start()

        def ours(i):
            with scope(f"sharewait{j}"):
                share(j, i).wait_recv()

            def one(t):
                x = panel[flat(j), :]
                mine = jnp.dot(x, w_in[:, columns(h, t)], preferred_element_type=F32)
                ssend[t, flat(j), :] = (mine + precv[t, flat(j), :].astype(F32)).astype(BF16)

            with scope(f"ours{j}"):
                each_tile(SLICES, j, i, one)
            cross(j, cut(SLICES, j, i), taken(j, i)).start()

        count = len(SLICES[j])
        theirs(0)
        for i in range(count):
            if i + 1 < count:
                theirs(i + 1)
            ours(i)

    def second(j):
        acc = total.at[pl.ds(0, counts[j])]
        acc[...] = jnp.zeros((counts[j], depth), F32)
        count = len(TAKEN[j])

        def down(i, which):
            def one(t):
                deep = pl.ds(pl.multiple_of(which * half + t * tile, tile), tile)
                acc[...] += jnp.dot(hidden[which, t, flat(j), :], w_out[deep, :], preferred_element_type=F32)

            with scope(f"down{j}"):
                each_tile(TAKEN, j, i, one)

        def theirs(i):
            with scope(f"spreadwait{j}"):
                spread(j, i, 1 - h).wait_recv()
            down(i, 1 - h)

        for i in range(count):
            with scope(f"crosswait{j}"):
                cross(j, cut(TAKEN, j, i), i).wait_recv()

            def activate(t):
                bias = b_in[:, pl.ds(pl.multiple_of(t * tile, tile), tile)]
                v = ssend[t, flat(j), :].astype(F32) + srecv[t, flat(j), :].astype(F32) + bias
                hidden[h, t, flat(j), :] = (v * (1.0 + lax.erf(v * (0.5**0.5))) * 0.5).astype(BF16)

            with scope(f"gelu{j}"):
                each_tile(TAKEN, j, i, activate)
            spread(j, i, h).start()
            if j == 0 and i == 0:
                load(1).wait()
            down(i, h)
            if i > 0:
                theirs(i - 1)
        theirs(count - 1)
        for cc, s in sorted(CHUNKS[j], reverse=True):
            held = total[pl.ds(base[cc, s] - starts[j], 4 * tall(s)), :]
            if cc == 0:
                okeep[quads(s), :] = held
            else:
                osend[quads(s), :] = held.astype(BF16)
                lend(s).start()

    def finish(s):
        summed = okeep[quads(s), :] + orecv[quads(s), :].astype(F32) + b_out[...]
        branch[quads(s), :] = summed.astype(BF16)
        for i in range(3):
            give(s, i).start()
        regrouped[r, span(s), :] = branch[part(4 * spans[s][0], s, r), :]

    def settle(s):
        for q in range(4):
            at = pl.ds(q * depth, depth)
            out_ref[span(s), at] = (
                tokens[span(s), at].astype(F32) + regrouped[q, span(s), :].astype(F32)
            ).astype(BF16)

    vector(0).wait()
    vector(1).start()
    flatten(gain_ref, gain, 0, width)
    for s in range(len(spans)):
        if s < 2:
            with scope(f"fetch{s}"):
                fetch(s).wait()
        with scope(f"norm{s}"):
            normalize(s)
        if s == 0:
            with scope("barrier"):
                pl.semaphore_wait(barrier, 4)
        for i in range(3):
            piece(s, i).start()
        panel[part(base[0, s], s, r), :] = normed[r, span(s), :]

    with scope("inwait0"):
        gathered(0, tall(0))
    forward(0).start()
    with scope("loadw"):
        load(0).wait()
    load(1).start()
    first(0)
    with scope("inwait1"):
        gathered(1, rows - tall(0))
    for s in range(1, last + 1):
        forward(s).start()
    with scope("fwdwait0"):
        passed(fwd_recv, 0, 0)
    first(1)
    with scope("fwdwait1"):
        passed(fwd_recv, 1, 1, 2)
    first(2)
    with scope("fwdwait3"):
        passed(fwd_recv, 2, 3)
    first(3)
    first(4)

    vector(1).wait()
    vector(2).start()
    flatten(b_in_ref, b_in, h * (half // 128), half)
    second(0)
    second(1)
    vector(2).wait()
    flatten(b_out_ref, b_out, 0, depth)
    with scope("lendwait0"):
        passed(o_recv, 0, 0)
    finish(0)
    second(2)
    with scope("lendwait1"):
        passed(o_recv, 1, 1, 2)
    finish(1)
    second(3)
    finish(2)
    second(4)
    with scope("lendwait3"):
        passed(o_recv, 2, 3)
    finish(3)
    with scope("givewait0"):
        gathered(0, rows - tall(last))
    for s in range(last):
        settle(s)
    with scope("givewait3"):
        gathered(1, tall(last))
    settle(last)

    with scope("drain"):
        for i, held in enumerate((panel.at[pl.ds(0, 6 * rows)], panel, hidden, psend)):
            remote(held, held, send_sem.at[i], send_sem.at[i], across).wait_send()


def fused(tokens, ln_gain, w_in, b_in, w_out, b_out):
    rows, width = tokens.shape
    depth, units = w_in.shape
    half = units // 2
    tile = tile_of(half, 512)
    spans, _, _, counts = plan(rows)
    cuts = sum(len(slices) for slices in TAKEN)
    vmem, dma = pltpu.VMEM, pltpu.SemaphoreType.DMA
    in_vmem, in_hbm = pl.BlockSpec(memory_space=vmem), pl.BlockSpec(memory_space=pl.ANY)
    stage = vmem((half // tile, 8 * rows, tile), BF16)
    return pl.pallas_call(
        block_kernel,
        out_shape=pltpu.VMEM((rows, width), BF16),
        in_specs=[in_hbm] * 6,
        out_specs=in_vmem,
        scratch_shapes=[
            vmem((rows, width), BF16),
            vmem((width // 128, 128), F32),
            vmem((units // 128, 128), F32),
            vmem((depth // 128, 128), F32),
            vmem((1, width), F32),
            vmem((1, half), F32),
            vmem((1, depth), F32),
            vmem(w_in.shape, BF16),
            vmem(w_out.shape, BF16),
            vmem((4, rows, depth), BF16),
            vmem((8 * rows, depth), BF16),
            stage,
            stage,
            stage,
            stage,
            vmem((2, half // tile, 8 * rows, tile), BF16),
            vmem((max(counts), depth), F32),
            vmem((4 * rows, depth), F32),
            vmem((4 * rows, depth), BF16),
            vmem((4 * rows, depth), BF16),
            vmem((4 * rows, depth), BF16),
            vmem((4, rows, depth), BF16),
            dma,
            dma((2,)),
            dma,
            dma((4,)),
            dma((2,)),
            dma((3,)),
            dma((4,)),
            dma((cuts,)),
            dma((4,)),
            dma((3,)),
        ],
        compiler_params=pltpu.CompilerParams(
            collective_id=0, has_side_effects=True, vmem_limit_bytes=62000000
        ),
        name="mlp_block",
    )(tokens, ln_gain.reshape(-1, 128), w_in, b_in.reshape(-1, 128), w_out, b_out.reshape(-1, 128))


def local(tokens, ln_gain, w_in, b_in, w_out, b_out):
    values = tokens.astype(jnp.float32)
    row_mean = jnp.mean(values, axis=1, keepdims=True)
    centered = values - row_mean
    row_var = jnp.mean(centered * centered, axis=1, keepdims=True)
    normed = (centered * lax.rsqrt(row_var + 1e-06) * ln_gain).astype(jnp.bfloat16)
    own_cols = lax.all_to_all(normed, "row", split_axis=1, concat_axis=0, tiled=True)
    partial_pre = jnp.dot(
        lax.all_gather(own_cols, "col", axis=0, tiled=True),
        w_in,
        preferred_element_type=jnp.float32,
    )
    preact = lax.psum_scatter(partial_pre, "row", scatter_dimension=0, tiled=True) + b_in
    hidden = jax.nn.gelu(preact, approximate=False).astype(jnp.bfloat16)
    down_part = jnp.dot(
        lax.all_gather(hidden, "row", axis=0, tiled=True), w_out, preferred_element_type=jnp.float32
    )
    summed = lax.psum_scatter(
        down_part.astype(jnp.bfloat16), "col", scatter_dimension=0, tiled=True
    ).astype(jnp.float32)
    branch_out = (summed + b_out).astype(jnp.bfloat16)
    regrouped = lax.all_to_all(branch_out, "row", split_axis=0, concat_axis=1, tiled=True)
    return (values + regrouped.astype(jnp.float32)).astype(jnp.bfloat16)


def solution(mesh):
    in_specs = (
        P(("grp", "row", "col"), None),
        P(),
        P("row", "col"),
        P("col"),
        P("col", "row"),
        P("row"),
    )
    out_specs = P(("grp", "row", "col"), None)
    body = fused if (mesh.shape["row"], mesh.shape["col"]) == (4, 2) else local
    return jax.shard_map(body, mesh=mesh, in_specs=in_specs, out_specs=out_specs, check_vma=False)
```
